16 devices in a mesh: rep: 1, dp: 16 (over x, y, z, core).
Axes of the slice: x: 2, y: 2, z: 2, core: 2. Of those that a mesh axis runs over, the one named last changes fastest.
Arguments:
- x: bfloat16 [16, 2048, 1024], P(('rep', 'dp'))
- dy: bfloat16 [16, 2048, 1024], P(('rep', 'dp'))
- w_gate: bfloat16 [2, 1024, 3328], P(None, 'dp')
- w_up: bfloat16 [2, 1024, 3328], P(None, 'dp')
- w_down: bfloat16 [2, 3328, 1024], P(None, 'dp')
- m_w_gate: float32 [2, 1024, 3328], P(None, 'dp')
- m_w_up: float32 [2, 1024, 3328], P(None, 'dp')
- m_w_down: float32 [2, 3328, 1024], P(None, 'dp')
- v_w_gate: float32 [2, 1024, 3328], P(None, 'dp')
- v_w_up: float32 [2, 1024, 3328], P(None, 'dp')
- v_w_down: float32 [2, 3328, 1024], P(None, 'dp')
Outputs:
- output 1: bfloat16 [2, 1024, 3328], P('rep', 'dp')
- output 2: bfloat16 [2, 1024, 3328], P('rep', 'dp')
- output 3: bfloat16 [2, 3328, 1024], P('rep', 'dp')
- output 4: float32 [2, 1024, 3328], P('rep', 'dp')
- output 5: float32 [2, 1024, 3328], P('rep', 'dp')
- output 6: float32 [2, 3328, 1024], P('rep', 'dp')
- output 7: float32 [2, 1024, 3328], P('rep', 'dp')
- output 8: float32 [2, 1024, 3328], P('rep', 'dp')
- output 9: float32 [2, 3328, 1024], P('rep', 'dp')
All inputs are finite; a program needn't handle non-finite values.
Results may differ from the reference program's by a relative error of at most 0.0224.
Values are sent between devices in bfloat16 or wider.
A program may use at most 2 GiB of HBM per device.

```python
import jax
import jax.numpy as jnp
from jax import lax

SEQUENCES = 16
TOKENS = 2048
D = 1024
FF = 3328
LAYERS = 2
NAMES = ("w_gate", "w_up", "w_down")
SHAPES = {"w_gate": (LAYERS, D, FF), "w_up": (LAYERS, D, FF), "w_down": (LAYERS, FF, D)}


def bump(key, n, height):
    away = (jnp.arange(n, dtype=jnp.int32) - jax.random.randint(key, (), 0, n, jnp.int32)) % n
    return jnp.where(away < n // 8, height, 1.0)


def together(key, own, strength):
    shared = jax.random.normal(key, own.shape[1:], jnp.float32)
    return (own + strength * shared) * lax.rsqrt(1 + strength * strength)


def setup_inputs(seed: int = 0, part: int = 0) -> dict:
    kx, kdy, ka, kb, kz, kf, kh, kl, *keys = jax.random.split(jax.random.key(seed), 8 + 3 * len(NAMES))
    kx, kdy, ka, kb = (jax.random.fold_in(k, part) for k in (kx, kdy, ka, kb))
    kw, km, kv = (keys[i::3] for i in range(3))
    shape = (SEQUENCES, TOKENS, D)
    much_x, much_dy = jax.random.uniform(kz, (2,), jnp.float32, 0.0, 1.0)
    loud = 2.0 ** jax.random.uniform(jax.random.fold_in(kz, 1), (), jnp.float32, -1.0, 2.0)
    layers = 2.0 ** jax.random.uniform(kl, (LAYERS, 1, 1), jnp.float32, -1.0, 1.0)
    x = together(ka, jax.random.normal(kx, shape, jnp.float32), much_x) * bump(kf, D, 4.0)
    dy = together(kb, jax.random.normal(kdy, shape, jnp.float32), much_dy)
    drawn = {"x": x.astype(jnp.bfloat16), "dy": (loud * dy * (SEQUENCES * TOKENS) ** -0.5).astype(jnp.bfloat16)}
    for key, name in zip(kw, NAMES, strict=True):
        w = jax.random.normal(key, SHAPES[name], jnp.float32) * SHAPES[name][1] ** -0.5
        drawn[name] = (w * {"w_gate": 1.0, "w_up": bump(kh, FF, 4.0), "w_down": layers}[name]).astype(jnp.bfloat16)
    for key, name in zip(km, NAMES, strict=True):
        drawn[f"m_{name}"] = 0.1 * jax.random.normal(key, SHAPES[name], jnp.float32)
    for key, name in zip(kv, NAMES, strict=True):
        drawn[f"v_{name}"] = jax.random.uniform(key, SHAPES[name], jnp.float32, 0.005, 0.015)
    return drawn


def matmul(a, w):
    return jnp.dot(a, w, preferred_element_type=jnp.float32).astype(jnp.bfloat16)


def normed(h):
    wide = h.astype(jnp.float32)
    scale = lax.rsqrt(jnp.mean(wide**2, -1, keepdims=True) + 1e-6)
    return (wide * scale).astype(jnp.bfloat16)


def layer(h, w):
    a = normed(h)
    gate = jnp.dot(a, w["w_gate"], preferred_element_type=jnp.float32)
    up = jnp.dot(a, w["w_up"], preferred_element_type=jnp.float32)
    return h + matmul((jax.nn.silu(gate) * up).astype(jnp.bfloat16), w["w_down"])


def adamw(w, m, v, g):
    m = 0.9 * m + 0.1 * g
    v = 0.95 * v + 0.05 * g * g
    step = m * lax.rsqrt(v + 1e-8) + 0.1 * w
    return (w - 0.02 * step).astype(jnp.bfloat16), m, v


def clipped(gradients, sum_of_squares, count):
    factor = jnp.minimum(1.0, 0.5 * lax.rsqrt(sum_of_squares / count + 1e-30))
    return [g * factor for g in gradients]


def stack(weights, h):
    return lax.scan(lambda h, w: (layer(h, w), None), h, weights)[0]


def reference(x, dy, w_gate, w_up, w_down, m_w_gate, m_w_up, m_w_down, v_w_gate, v_w_up, v_w_down):
    weights = dict(zip(NAMES, (w_gate, w_up, w_down), strict=True))

    def take(so_far, sequence):
        h, by_y = sequence
        _, back = jax.vjp(lambda w: stack(w, h), weights)
        return jax.tree.map(lambda total, term: total + term.astype(jnp.float32), so_far, back(by_y)[0]), None

    none_yet = {name: jnp.zeros(w.shape, jnp.float32) for name, w in weights.items()}
    by_weights, _ = lax.scan(take, none_yet, (x, dy))
    gradients = [by_weights[name].astype(jnp.bfloat16).astype(jnp.float32) for name in NAMES]
    gradients = clipped(gradients, sum(jnp.sum(g * g) for g in gradients), sum(g.size for g in gradients))
    new = [
        adamw(w.astype(jnp.float32), m, v, g)
        for w, m, v, g in zip((w_gate, w_up, w_down), (m_w_gate, m_w_up, m_w_down), (v_w_gate, v_w_up, v_w_down), gradients, strict=True)
    ]
    return tuple(one[which] for which in range(3) for one in new)
```

```python
import functools

import jax
import jax.numpy as jnp
from jax import lax
from jax.experimental import pallas as pl
from jax.experimental.pallas import tpu as pltpu
from jax.sharding import PartitionSpec as P

NAMES = ("w_gate", "w_up", "w_down")
BF, F32 = jnp.bfloat16, jnp.float32
ORDERS = ((0, 1, 2), (1, 2, 0), (2, 0, 1))
ANY = pl.BlockSpec(memory_space=pl.ANY)
VMEM = pl.BlockSpec(memory_space=pltpu.VMEM)


def spot():
    me = lax.axis_index("dp")
    return me, ((me // 8) % 2, (me // 4) % 2, (me // 2) % 2, me % 2)


def peer(axis):
    me, bits = spot()
    return {"dp": me + (1 - 2 * bits[axis]) * (8 >> axis)}


def greet():
    barrier = pltpu.get_barrier_semaphore()
    for axis in range(4):
        pl.semaphore_signal(barrier, inc=1, device_id=peer(axis), device_id_type=pl.DeviceIdType.MESH)
    pl.semaphore_wait(barrier, 4)


def thirds(columns, turn=0):
    tiles = columns // 128
    sizes = [tiles // 3 + (i < tiles % 3) for i in range(3)]
    parts, at = [], 0
    for i, size in enumerate(sizes):
        parts.append((pl.ds(at * 128, size * 128), size * 128, ORDERS[(i + turn) % 3]))
        at += size
    return parts


def send(src, dst, send_sem, recv_sem, axis):
    return pltpu.make_async_remote_copy(
        src_ref=src, dst_ref=dst, send_sem=send_sem, recv_sem=recv_sem, device_id=peer(axis), device_id_type=pl.DeviceIdType.MESH
    )


class Gather:
    scratch = [pltpu.SemaphoreType.DMA((3, 3, 2)), pltpu.SemaphoreType.DMA((2,)), pltpu.SemaphoreType.DMA]

    def __init__(self, own, whole, sems, turn=0):
        self.own, self.whole, (self.sems, self.side, self.local) = own, whole, sems
        self.parts = thirds(own.shape[-1], turn)
        _, self.bits = spot()

    def at(self, cols, done, flip=None):
        index = [slice(None) if a in done else self.bits[a] for a in range(4)]
        if flip is not None:
            index[flip] = 1 - self.bits[flip]
        return self.whole.at[(*index, slice(None), cols)]

    def place(self):
        return pltpu.make_async_copy(self.own, self.at(slice(None), ()), self.local)

    def hop(self, p, phase):
        cols, _, order = self.parts[p]
        here = self.at(cols, order[:phase])
        return send(self.own.at[:, cols] if phase == 0 else here, here, self.sems.at[p, phase, 0], self.sems.at[p, phase, 1], order[phase])

    def across(self, src):
        return lambda dst: send(src, dst, self.side.at[0], self.side.at[1], 3)

    def stages(self):
        def begin():
            self.place().start()
            for p in range(3):
                self.hop(p, 0).start()
            self.across(self.own)(self.at(slice(None), ())).start()

        def go_on(phase):
            def run():
                if phase == 1:
                    self.place().wait()
                for p, (cols, _, order) in enumerate(self.parts):
                    self.hop(p, phase - 1).wait()
                    if phase < 3:
                        self.hop(p, phase).start()
                    got = self.at(cols, order[: phase - 1], order[phase - 1])
                    self.across(got)(got).start()

            return run

        def end():
            half = self.at(slice(None), (0, 1, 2))
            self.across(half)(half).wait()

        return [begin, go_on(1), go_on(2), go_on(3), end]


class Scatter:
    @staticmethod
    def scratch(rows, columns):
        return [
            pltpu.VMEM((2, 2, 2, rows, columns), BF),
            pltpu.VMEM((2, 2, 2, rows, columns), BF),
            pltpu.VMEM((4, rows, columns), BF),
            pltpu.VMEM((2, rows, columns), BF),
            pltpu.VMEM((1, rows, columns), BF),
            pltpu.SemaphoreType.DMA((3, 4, 2)),
            pltpu.SemaphoreType.DMA,
        ]

    def __init__(self, whole, mine, scratch, turn=0):
        self.whole, self.mine = whole, mine
        self.own, *self.got, self.sems, self.local = scratch
        self.parts = thirds(whole.shape[-1], turn)
        _, self.bits = spot()

    def index(self, done, flip=None):
        index = [self.bits[a] if a in done else slice(None) for a in range(3)]
        if flip is not None:
            index[flip] = 1 - self.bits[flip]
        return tuple(index)

    def load(self):
        return pltpu.make_async_copy(self.whole.at[:, :, :, self.bits[3]], self.own, self.local)

    def first(self, p):
        cols = self.parts[p][0]
        return send(
            self.whole.at[:, :, :, 1 - self.bits[3], :, cols],
            self.got[0].at[:, :, :, :, cols],
            self.sems.at[p, 0, 0],
            self.sems.at[p, 0, 1],
            3,
        )

    def blocks(self, p, phase):
        order = self.parts[p][2]
        free = order[phase:]
        for k in range(2 ** len(free)):
            index = [self.bits[a] for a in range(3)]
            index[order[phase - 1]] = 1 - self.bits[order[phase - 1]]
            for i, a in enumerate(free):
                index[a] = (k >> (len(free) - 1 - i)) & 1
            yield tuple(index), k

    def hops(self, p, phase):
        cols = self.parts[p][0]
        order = self.parts[p][2]
        for index, k in self.blocks(p, phase):
            yield send(
                self.own.at[(*index, slice(None), cols)],
                self.got[phase].at[k, :, cols],
                self.sems.at[p, phase, 0],
                self.sems.at[p, phase, 1],
                order[phase - 1],
            )

    def landed(self, p, phase):
        cols = self.parts[p][0]
        whole = self.got[phase].at[:, :, cols]
        return send(whole, whole, self.sems.at[p, phase, 0], self.sems.at[p, phase, 1], self.parts[p][2][phase - 1])

    def total(self, p, index, upto):
        cols, _, order = self.parts[p]
        value = self.own[(*index, slice(None), cols)].astype(F32) + self.got[0][(*index, slice(None), cols)].astype(F32)
        for phase in range(1, upto):
            place = 0
            for a in order[phase:]:
                place = 2 * place + index[a]
            value += self.got[phase][place, :, cols].astype(F32)
        return value

    def stages(self):
        def begin():
            self.load().start()
            for p in range(3):
                self.first(p).start()

        def add(phase):
            def run():
                if phase == 1:
                    self.load().wait()
                for p, (cols, _, _) in enumerate(self.parts):
                    if phase == 1:
                        self.first(p).wait()
                    else:
                        self.landed(p, phase - 1).wait()
                    for index, _ in self.blocks(p, phase):
                        self.own[(*index, slice(None), cols)] = self.total(p, index, phase).astype(BF)
                    for hop in self.hops(p, phase):
                        hop.start()

            return run

        def end():
            for p, (cols, _, _) in enumerate(self.parts):
                self.landed(p, 3).wait()
                self.mine[:, cols] = self.total(p, self.bits[:3], 4).astype(BF)

        return [begin, add(1), add(2), add(3), end]


def interleave(jobs, lag=1):
    lists = [job.stages() for job in jobs]
    for t in range(max(len(s) + lag * j for j, s in enumerate(lists))):
        for j, s in reversed(list(enumerate(lists))):
            if 0 <= t - lag * j < len(s):
                s[t - lag * j]()


def chunked(refs, sizes):
    out, at = [], 0
    for size in sizes:
        out.append(refs[at : at + size])
        at += size
    return out


def gather_all(weights, identity):
    layers, n = weights[0].shape[0], len(weights)

    def kernel(*refs):
        own, whole, scratch = refs[:n], refs[n : n + n * layers], refs[n + n * layers :]
        greet()
        scratch = chunked(scratch, [3] * (n * layers))
        interleave([Gather(own[i % n].at[i // n], whole[i], scratch[i], i) for i in range(n * layers)])

    out = pl.pallas_call(
        kernel,
        in_specs=[VMEM] * n,
        out_specs=[ANY] * (n * layers),
        out_shape=[jax.ShapeDtypeStruct((2, 2, 2, 2, *w.shape[1:]), BF) for _ in range(layers) for w in weights],
        scratch_shapes=Gather.scratch * (n * layers),
        compiler_params=pltpu.CompilerParams(collective_id=identity, has_side_effects=True, vmem_limit_bytes=60 << 20),
    )(*weights)
    out = [w.reshape(16 * w.shape[4], w.shape[5]) for w in out]
    return [dict(zip(NAMES, out[n * i : n * i + n])) for i in range(layers)]


def scatter_all(terms, identity):
    n = len(terms)
    terms = [t.reshape(2, 2, 2, 2, t.shape[0] // 16, t.shape[1]) for t in terms]

    def kernel(*refs):
        whole, mine, scratch = refs[:n], refs[n : 2 * n], refs[2 * n :]
        greet()
        scratch = chunked(scratch, [7] * n)
        interleave([Scatter(whole[i], mine[i], scratch[i], i) for i in range(n)])

    return pl.pallas_call(
        kernel,
        in_specs=[ANY] * n,
        out_specs=[VMEM] * n,
        out_shape=[jax.ShapeDtypeStruct(t.shape[4:], BF) for t in terms],
        scratch_shapes=[s for t in terms for s in Scatter.scratch(*t.shape[4:])],
        compiler_params=pltpu.CompilerParams(collective_id=identity, has_side_effects=True, vmem_limit_bytes=60 << 20),
    )(*terms)


def sum_of_squares(gradients, identity):
    n = len(gradients)

    def kernel(*refs):
        ours, out, term, slots, sems = refs[:n], *refs[n:]
        me, _ = spot()
        barrier = pltpu.get_barrier_semaphore()
        for k in range(1, 16):
            pl.semaphore_signal(barrier, inc=1, device_id={"dp": (me + k) % 16}, device_id_type=pl.DeviceIdType.MESH)
        pl.semaphore_wait(barrier, 15)
        total = jnp.zeros((8, 128), F32)
        for g in ours:
            rows, columns = g.shape

            def add(i, total, g=g, columns=columns):
                wide = g[pl.ds(pl.multiple_of(i * 16, 16), 16), :].astype(F32)
                wide = wide * wide
                for j in range(columns // 128):
                    total = total + wide[:8, 128 * j : 128 * j + 128] + wide[8:, 128 * j : 128 * j + 128]
                return total

            total = lax.fori_loop(0, rows // 16, add, total)
        term[...] = total
        copies = [
            pltpu.make_async_remote_copy(
                src_ref=term,
                dst_ref=slots.at[k - 1],
                send_sem=sems.at[k - 1, 0],
                recv_sem=sems.at[k - 1, 1],
                device_id={"dp": (me + k) % 16},
                device_id_type=pl.DeviceIdType.MESH,
            )
            for k in range(1, 16)
        ]
        for copy in copies:
            copy.start()
        for copy in copies:
            copy.wait()
        total = term[...]
        for k in range(15):
            total = total + slots[k]
        out[...] = total

    return pl.pallas_call(
        kernel,
        in_specs=[VMEM] * n,
        out_specs=VMEM,
        out_shape=jax.ShapeDtypeStruct((8, 128), F32),
        scratch_shapes=[pltpu.VMEM((8, 128), F32), pltpu.VMEM((15, 8, 128), F32), pltpu.SemaphoreType.DMA((15, 2))],
        compiler_params=pltpu.CompilerParams(collective_id=identity, has_side_effects=True),
    )(*gradients)


def matmul(a, w):
    return jnp.dot(a, w, preferred_element_type=F32).astype(BF)


def normed(h):
    wide = h.astype(F32)
    scale = lax.rsqrt(jnp.mean(wide**2, -1, keepdims=True) + 1e-6)
    return (wide * scale).astype(BF)


def layer(h, w):
    a = normed(h)
    gate = jnp.dot(a, w["w_gate"], preferred_element_type=F32)
    up = jnp.dot(a, w["w_up"], preferred_element_type=F32)
    return h + matmul((jax.nn.silu(gate) * up).astype(BF), w["w_down"])


def adamw(w, m, v, g):
    m = 0.9 * m + 0.1 * g
    v = 0.95 * v + 0.05 * g * g
    step = m * lax.rsqrt(v + 1e-8) + 0.1 * w
    return (w - 0.02 * step).astype(BF), m, v


def solution(mesh):
    def step(x, dy, *arrays):
        weights, m, v = (arrays[i : i + 3] for i in (0, 3, 6))
        layers = weights[0].shape[0]
        whole = gather_all(weights, 0)
        h, kept = x[0], []
        for number in range(layers):
            kept.append(h)
            h = layer(h, whole[number])
        by_h, mine = dy[0], [None] * layers
        for number in reversed(range(layers)):
            _, back = jax.vjp(lambda w, h: layer(h, w), whole[number], kept[number])
            by_w, by_h = back(by_h)
            mine[number] = scatter_all([by_w[name] for name in NAMES], 1 + number)
        squares = jnp.sum(sum_of_squares([g for one in mine for g in one], 1 + layers))
        gradients = [jnp.stack([mine[number][i] for number in range(layers)]).astype(F32) for i in range(3)]
        factor = jnp.minimum(1.0, 0.5 * lax.rsqrt(squares / (16 * sum(g.size for g in gradients)) + 1e-30))
        new = [adamw(w.astype(F32), m, v, g * factor) for w, m, v, g in zip(weights, m, v, gradients, strict=True)]
        return tuple(one[which] for which in range(3) for one in new)

    states, cut = P(("rep", "dp"), None, None), P(None, "dp", None)
    return jax.shard_map(
        step,
        mesh=mesh,
        in_specs=(states, states) + (cut,) * 9,
        out_specs=(P("rep", "dp", None),) * 9,
        check_vma=False,
    )
```

```python
import functools

import jax
import jax.numpy as jnp
from jax import lax
from jax.experimental import pallas as pl
from jax.experimental.pallas import tpu as pltpu
from jax.sharding import PartitionSpec as P

NAMES = ("w_gate", "w_up", "w_down")
BF, F32 = jnp.bfloat16, jnp.float32
ORDERS = ((0, 1, 2), (1, 2, 0), (2, 0, 1))
ANY = pl.BlockSpec(memory_space=pl.ANY)
VMEM = pl.BlockSpec(memory_space=pltpu.VMEM)


def spot():
    me = lax.axis_index("dp")
    return me, ((me // 8) % 2, (me // 4) % 2, (me // 2) % 2, me % 2)


def peer(axis):
    me, bits = spot()
    return {"dp": me + (1 - 2 * bits[axis]) * (8 >> axis)}


def greet():
    barrier = pltpu.get_barrier_semaphore()
    for axis in range(4):
        pl.semaphore_signal(barrier, inc=1, device_id=peer(axis), device_id_type=pl.DeviceIdType.MESH)
    pl.semaphore_wait(barrier, 4)


def thirds(columns, turn=0):
    tiles = columns // 128
    sizes = [tiles // 3 + (i < tiles % 3) for i in range(3)]
    parts, at = [], 0
    for i, size in enumerate(sizes):
        parts.append((pl.ds(at * 128, size * 128), size * 128, ORDERS[(i + turn) % 3]))
        at += size
    return parts


def send(src, dst, send_sem, recv_sem, axis):
    return pltpu.make_async_remote_copy(
        src_ref=src, dst_ref=dst, send_sem=send_sem, recv_sem=recv_sem, device_id=peer(axis), device_id_type=pl.DeviceIdType.MESH
    )


class Gather:
    scratch = [pltpu.SemaphoreType.DMA((3, 3, 2)), pltpu.SemaphoreType.DMA((2,)), pltpu.SemaphoreType.DMA]

    def __init__(self, own, whole, sems, turn=0):
        self.own, self.whole, (self.sems, self.side, self.local) = own, whole, sems
        self.parts = thirds(own.shape[-1], turn)
        _, self.bits = spot()

    def at(self, cols, done, flip=None):
        index = [slice(None) if a in done else self.bits[a] for a in range(4)]
        if flip is not None:
            index[flip] = 1 - self.bits[flip]
        return self.whole.at[(*index, slice(None), cols)]

    def place(self):
        return pltpu.make_async_copy(self.own, self.at(slice(None), ()), self.local)

    def hop(self, p, phase):
        cols, _, order = self.parts[p]
        here = self.at(cols, order[:phase])
        return send(self.own.at[:, cols] if phase == 0 else here, here, self.sems.at[p, phase, 0], self.sems.at[p, phase, 1], order[phase])

    def across(self, src):
        return lambda dst: send(src, dst, self.side.at[0], self.side.at[1], 3)

    def stages(self):
        def begin():
            self.place().start()
            for p in range(3):
                self.hop(p, 0).start()
            self.across(self.own)(self.at(slice(None), ())).start()

        def go_on(phase):
            def run():
                if phase == 1:
                    self.place().wait()
                for p, (cols, _, order) in enumerate(self.parts):
                    self.hop(p, phase - 1).wait()
                    if phase < 3:
                        self.hop(p, phase).start()
                    got = self.at(cols, order[: phase - 1], order[phase - 1])
                    self.across(got)(got).start()

            return run

        def end():
            half = self.at(slice(None), (0, 1, 2))
            self.across(half)(half).wait()

        return [begin, go_on(1), go_on(2), go_on(3), end]


class Scatter:
    @staticmethod
    def scratch(rows, columns):
        return [
            pltpu.VMEM((2, 2, 2, rows, columns), BF),
            pltpu.VMEM((2, 2, 2, rows, columns), BF),
            pltpu.VMEM((4, rows, columns), BF),
            pltpu.VMEM((2, rows, columns), BF),
            pltpu.VMEM((1, rows, columns), BF),
            pltpu.SemaphoreType.DMA((3, 4, 2)),
            pltpu.SemaphoreType.DMA,
        ]

    def __init__(self, whole, mine, scratch, turn=0):
        self.whole, self.mine = whole, mine
        self.own, *self.got, self.sems, self.local = scratch
        self.parts = thirds(whole.shape[-1], turn)
        _, self.bits = spot()

    def index(self, done, flip=None):
        index = [self.bits[a] if a in done else slice(None) for a in range(3)]
        if flip is not None:
            index[flip] = 1 - self.bits[flip]
        return tuple(index)

    def load(self):
        return pltpu.make_async_copy(self.whole.at[:, :, :, self.bits[3]], self.own, self.local)

    def first(self, p):
        cols = self.parts[p][0]
        return send(
            self.whole.at[:, :, :, 1 - self.bits[3], :, cols],
            self.got[0].at[:, :, :, :, cols],
            self.sems.at[p, 0, 0],
            self.sems.at[p, 0, 1],
            3,
        )

    def blocks(self, p, phase):
        order = self.parts[p][2]
        free = order[phase:]
        for k in range(2 ** len(free)):
            index = [self.bits[a] for a in range(3)]
            index[order[phase - 1]] = 1 - self.bits[order[phase - 1]]
            for i, a in enumerate(free):
                index[a] = (k >> (len(free) - 1 - i)) & 1
            yield tuple(index), k

    def hops(self, p, phase):
        cols = self.parts[p][0]
        order = self.parts[p][2]
        for index, k in self.blocks(p, phase):
            yield send(
                self.own.at[(*index, slice(None), cols)],
                self.got[phase].at[k, :, cols],
                self.sems.at[p, phase, 0],
                self.sems.at[p, phase, 1],
                order[phase - 1],
            )

    def landed(self, p, phase):
        cols = self.parts[p][0]
        whole = self.got[phase].at[:, :, cols]
        return send(whole, whole, self.sems.at[p, phase, 0], self.sems.at[p, phase, 1], self.parts[p][2][phase - 1])

    def total(self, p, index, upto):
        cols, _, order = self.parts[p]
        value = self.own[(*index, slice(None), cols)].astype(F32) + self.got[0][(*index, slice(None), cols)].astype(F32)
        for phase in range(1, upto):
            place = 0
            for a in order[phase:]:
                place = 2 * place + index[a]
            value += self.got[phase][place, :, cols].astype(F32)
        return value

    def stages(self):
        def begin():
            self.load().start()
            for p in range(3):
                self.first(p).start()

        def add(phase):
            def run():
                if phase == 1:
                    self.load().wait()
                for p, (cols, _, _) in enumerate(self.parts):
                    if phase == 1:
                        self.first(p).wait()
                    else:
                        self.landed(p, phase - 1).wait()
                    for index, _ in self.blocks(p, phase):
                        self.own[(*index, slice(None), cols)] = self.total(p, index, phase).astype(BF)
                    for hop in self.hops(p, phase):
                        hop.start()

            return run

        def end():
            for p, (cols, _, _) in enumerate(self.parts):
                self.landed(p, 3).wait()
                self.mine[:, cols] = self.total(p, self.bits[:3], 4).astype(BF)

        return [begin, add(1), add(2), add(3), end]


def interleave(jobs, lag=1):
    lists = [job.stages() for job in jobs]
    for t in range(max(len(s) + lag * j for j, s in enumerate(lists))):
        for j, s in reversed(list(enumerate(lists))):
            if 0 <= t - lag * j < len(s):
                s[t - lag * j]()


def chunked(refs, sizes):
    out, at = [], 0
    for size in sizes:
        out.append(refs[at : at + size])
        at += size
    return out


def normed(h):
    wide = h.astype(F32)
    scale = lax.rsqrt(jnp.mean(wide**2, -1, keepdims=True) + 1e-6)
    return (wide * scale).astype(BF)


def dot(a, b, over=(1, 0)):
    return lax.dot_general(a, b, (((over[0],), (over[1],)), ((), ())), preferred_element_type=F32)


class Gathers:
    def __init__(self, own, picks):
        self.args, self.picks = list(own), picks
        self.in_specs = [VMEM] * len(own)
        self.out_shape = [jax.ShapeDtypeStruct((2, 2, 2, 2, *own[i].shape[1:]), BF) for i, _ in picks]
        self.out_specs = [ANY] * len(picks)
        self.scratch = Gather.scratch * len(picks)

    def jobs(self, ins, outs, scratch):
        scratch = chunked(scratch, [3] * len(self.picks))
        return [Gather(ins[i].at[number], outs[n], scratch[n], n) for n, (i, number) in enumerate(self.picks)]

    @staticmethod
    def finished(outs):
        return [w.reshape(16 * w.shape[4], w.shape[5]) for w in outs]


class Scatters:
    def __init__(self, terms):
        self.args = [t.reshape(2, 2, 2, 2, t.shape[0] // 16, t.shape[1]) for t in terms]
        self.in_specs = [ANY] * len(terms)
        self.out_shape = [jax.ShapeDtypeStruct(t.shape[4:], BF) for t in self.args]
        self.out_specs = [VMEM] * len(terms)
        self.scratch = [s for t in self.args for s in Scatter.scratch(*t.shape[4:])]

    def jobs(self, ins, outs, scratch):
        scratch = chunked(scratch, [7] * len(self.args))
        return [Scatter(ins[n], outs[n], scratch[n], n) for n in range(len(self.args))]

    @staticmethod
    def finished(outs):
        return list(outs)


class Nothing:
    args, in_specs, out_shape, out_specs, scratch = [], [], [], [], []

    @staticmethod
    def finished(outs):
        return []


def call(name, identity, steps, body, args, in_specs, out_shape, out_specs, scratch, traffic, times):
    counts = [len(args), len(traffic.args), len(out_shape), len(traffic.out_shape), len(scratch), len(traffic.scratch)]

    def kernel(*refs):
        ins, t_ins, outs, t_outs, own, t_scratch = chunked(refs, counts)
        step = pl.program_id(0)
        plan = []
        if traffic.args:
            for n, (job, when) in enumerate(zip(traffic.jobs(t_ins, t_outs, t_scratch), times, strict=True)):
                plan += [(at, -n, stage) for at, stage in zip(when, job.stages(), strict=True)]
            plan.sort(key=lambda one: one[:2])

        def run(at, first=False):
            now = [stage for when, _, stage in plan if (when == at if at < steps else when >= steps)]
            if now or first:

                @pl.when(step == min(at, steps - 1))
                def _():
                    if first and plan:
                        greet()
                    for stage in now:
                        stage()

        for at in range(steps):
            run(at, at == 0)
        body(step, ins, outs, own)
        run(steps)

    params = dict(vmem_limit_bytes=62 << 20, dimension_semantics=("arbitrary",))
    if traffic.args:
        params |= dict(collective_id=identity, has_side_effects=True)
    out = pl.pallas_call(
        kernel,
        name=name,
        grid=(steps,),
        in_specs=in_specs + traffic.in_specs,
        out_specs=out_specs + traffic.out_specs,
        out_shape=out_shape + traffic.out_shape,
        scratch_shapes=scratch + traffic.scratch,
        compiler_params=pltpu.CompilerParams(**params),
    )(*args, *traffic.args)
    return (*out[: len(out_shape)], traffic.finished(out[len(out_shape) :]))


def fixed(shape):
    return pl.BlockSpec(shape, lambda i: (0,) * len(shape), pipeline_mode=pl.Buffered(1))


def down(shape):
    return pl.BlockSpec(shape, lambda i: (i, 0))


def along(shape):
    return pl.BlockSpec(shape, lambda i: (0, i))


def like(shape, dtype=BF):
    return jax.ShapeDtypeStruct(shape, dtype)


WIDE = 256
TALL = 256


def start(x, identity, traffic, times):
    tokens, d = x.shape
    rows = tokens // 8

    def body(step, ins, outs, _):
        outs[0][...] = normed(ins[0][...])

    spec = down((rows, d))
    return call("start", identity, 8, body, [x], [spec], [like(x.shape)], [spec], [], traffic, times)


def gate_up(a, w_gate, w_up, identity, traffic, times):
    tokens, d = a.shape
    ff = w_gate.shape[1]
    cut = tokens // 4

    def body(step, ins, outs, _):
        a, w_gate, w_up = ins
        hidden, by_gate, by_up = outs
        for i in range(0, tokens, cut):
            rows = pl.ds(i, cut)
            gate = dot(a[rows, :], w_gate[...])
            up = dot(a[rows, :], w_up[...])
            sigmoid = 1.0 / (1.0 + jnp.exp(-gate))
            silu = gate * sigmoid
            hidden[rows, :] = (silu * up).astype(BF)
            by_gate[rows, :] = up * (sigmoid + silu * (1.0 - sigmoid))
            by_up[rows, :] = silu

    out = along((tokens, WIDE))
    return call(
        "gate_up",
        identity,
        ff // WIDE,
        body,
        [a, w_gate, w_up],
        [fixed(a.shape)] + [along((d, WIDE))] * 2,
        [like((tokens, ff)), like((tokens, ff), F32), like((tokens, ff), F32)],
        [out] * 3,
        [],
        traffic,
        times,
    )


def back_down(h, hidden, w_down, identity, traffic, times):
    tokens, d = h.shape
    ff = hidden.shape[1]

    def body(step, ins, outs, _):
        h, hidden, w_down = ins
        states = h[...] + dot(hidden[...], w_down[...]).astype(BF)
        outs[0][...] = states
        outs[1][...] = normed(states)

    return call(
        "down",
        identity,
        tokens // TALL,
        body,
        [h, hidden, w_down],
        [down((TALL, d)), down((TALL, ff)), fixed(w_down.shape)],
        [like(h.shape)] * 2,
        [down((TALL, d))] * 2,
        [],
        traffic,
        times,
    )


def by_hidden(by_h, hidden, by_gate, by_up, w_down, identity, traffic, times):
    tokens, d = by_h.shape
    ff = hidden.shape[1]
    cut = tokens // 4

    def body(step, ins, outs, _):
        by_h, hidden, by_gate, by_up, w_down = ins
        gate, up, term = outs
        for i in range(0, tokens, cut):
            rows = pl.ds(i, cut)
            wide = dot(by_h[rows, :], w_down[...], (1, 1)).astype(BF).astype(F32)
            gate[rows, :] = (wide * by_gate[rows, :]).astype(BF)
            up[rows, :] = (wide * by_up[rows, :]).astype(BF)
        term[...] = dot(hidden[...], by_h[...], (0, 0)).astype(BF)

    block = along((tokens, WIDE))
    return call(
        "by_hidden",
        identity,
        ff // WIDE,
        body,
        [by_h, hidden, by_gate, by_up, w_down],
        [fixed(by_h.shape), block, block, block, down((WIDE, d))],
        [like((tokens, ff))] * 2 + [like((ff, d))],
        [block, block, down((WIDE, d))],
        [],
        traffic,
        times,
    )


def by_weights(a, gate, up, identity, traffic, times):
    tokens, d = a.shape
    ff = gate.shape[1]

    def body(step, ins, outs, scratch):
        a, gate, up = ins
        turned = scratch[0]

        @pl.when(step == 0)
        def _():
            for i in range(0, tokens, 256):
                turned[:, i : i + 256] = a[i : i + 256, :].T

        outs[0][...] = dot(turned[...], gate[...]).astype(BF)
        outs[1][...] = dot(turned[...], up[...]).astype(BF)

    block = along((tokens, WIDE))
    return call(
        "by_weights",
        identity,
        ff // WIDE,
        body,
        [a, gate, up],
        [fixed(a.shape), block, block],
        [like((d, ff))] * 2,
        [along((d, WIDE))] * 2,
        [pltpu.VMEM((d, tokens), BF)],
        traffic,
        times,
    )


def by_states(h, by_h, gate, up, w_gate, w_up, identity, traffic, times):
    tokens, d = h.shape
    ff = gate.shape[1]

    def body(step, ins, outs, _):
        h, by_h, gate, up, w_gate, w_up = ins
        by_a = dot(gate[...], w_gate[...], (1, 1)).astype(BF) + dot(up[...], w_up[...], (1, 1)).astype(BF)
        by_a, wide = by_a.astype(F32), h[...].astype(F32)
        scale = lax.rsqrt(jnp.mean(wide**2, -1, keepdims=True) + 1e-6)
        by_wide = scale * by_a - wide * (scale * scale * scale * jnp.mean(by_a * wide, -1, keepdims=True))
        outs[0][...] = by_h[...] + by_wide.astype(BF)

    states, block = down((TALL, d)), down((TALL, ff))
    return call(
        "by_states",
        identity,
        tokens // TALL,
        body,
        [h, by_h, gate, up, w_gate, w_up],
        [states, states, block, block, fixed(w_gate.shape), fixed(w_up.shape)],
        [like(h.shape)],
        [states],
        [],
        traffic,
        times,
    )


def scatter_all(terms, identity):
    n = len(terms)
    terms = [t.reshape(2, 2, 2, 2, t.shape[0] // 16, t.shape[1]) for t in terms]

    def kernel(*refs):
        whole, mine, scratch = refs[:n], refs[n : 2 * n], refs[2 * n :]
        greet()
        scratch = chunked(scratch, [7] * n)
        interleave([Scatter(whole[i], mine[i], scratch[i], i) for i in range(n)])

    return pl.pallas_call(
        kernel,
        in_specs=[ANY] * n,
        out_specs=[VMEM] * n,
        out_shape=[jax.ShapeDtypeStruct(t.shape[4:], BF) for t in terms],
        scratch_shapes=[s for t in terms for s in Scatter.scratch(*t.shape[4:])],
        compiler_params=pltpu.CompilerParams(collective_id=identity, has_side_effects=True, vmem_limit_bytes=60 << 20),
    )(*terms)


def sum_of_squares(gradients, identity):
    n = len(gradients)

    def kernel(*refs):
        ours, out, term, slots, sems = refs[:n], *refs[n:]
        me, _ = spot()
        barrier = pltpu.get_barrier_semaphore()
        for k in range(1, 16):
            pl.semaphore_signal(barrier, inc=1, device_id={"dp": (me + k) % 16}, device_id_type=pl.DeviceIdType.MESH)
        pl.semaphore_wait(barrier, 15)
        total = jnp.zeros((8, 128), F32)
        for g in ours:
            rows, columns = g.shape

            def add(i, total, g=g, columns=columns):
                wide = g[pl.ds(pl.multiple_of(i * 16, 16), 16), :].astype(F32)
                wide = wide * wide
                for j in range(columns // 128):
                    total = total + wide[:8, 128 * j : 128 * j + 128] + wide[8:, 128 * j : 128 * j + 128]
                return total

            total = lax.fori_loop(0, rows // 16, add, total)
        term[...] = total
        copies = [
            pltpu.make_async_remote_copy(
                src_ref=term,
                dst_ref=slots.at[k - 1],
                send_sem=sems.at[k - 1, 0],
                recv_sem=sems.at[k - 1, 1],
                device_id={"dp": (me + k) % 16},
                device_id_type=pl.DeviceIdType.MESH,
            )
            for k in range(1, 16)
        ]
        for copy in copies:
            copy.start()
        for copy in copies:
            copy.wait()
        total = term[...]
        for k in range(15):
            total = total + slots[k]
        out[...] = total

    return pl.pallas_call(
        kernel,
        in_specs=[VMEM] * n,
        out_specs=VMEM,
        out_shape=jax.ShapeDtypeStruct((8, 128), F32),
        scratch_shapes=[pltpu.VMEM((8, 128), F32), pltpu.VMEM((15, 8, 128), F32), pltpu.SemaphoreType.DMA((15, 2))],
        compiler_params=pltpu.CompilerParams(collective_id=identity, has_side_effects=True),
    )(*gradients)


def adamw(w, m, v, g):
    m = 0.9 * m + 0.1 * g
    v = 0.95 * v + 0.05 * g * g
    step = m * lax.rsqrt(v + 1e-8) + 0.1 * w
    return (w - 0.02 * step).astype(BF), m, v


def solution(mesh):
    def step(x, dy, *arrays):
        weights, m, v = (arrays[i : i + 3] for i in (0, 3, 6))
        w_gate, w_up, w_down = weights
        layers = w_gate.shape[0]
        x, dy = x[0], dy[0]
        a0, (wg0, wu0) = start(x, 0, Gathers((w_gate, w_up), [(0, 0), (1, 0)]), [(0, 1, 2, 3, 8), (1, 2, 3, 8, 9)])
        hid0, g0, u0, (wd0, wg1) = gate_up(
            a0, wg0, wu0, 1, Gathers((w_down, w_gate), [(0, 0), (1, 1)]), [(0, 2, 5, 9, 13), (1, 4, 8, 13, 14)]
        )
        h1, a1, (wu1,) = back_down(x, hid0, wd0, 2, Gathers((w_up,), [(0, 1)]), [(0, 2, 4, 8, 9)])
        hid1, g1, u1, (wd1,) = gate_up(a1, wg1, wu1, 3, Gathers((w_down,), [(0, 1)]), [(0, 2, 5, 10, 13)])
        dg1, du1, term_d1, _ = by_hidden(dy, hid1, g1, u1, wd1, 4, Nothing, ())
        term_g1, term_u1, (d1,) = by_weights(a1, dg1, du1, 5, Scatters([term_d1]), [(0, 3, 8, 11, 13)])
        by_h1, (sg1,) = by_states(h1, dy, dg1, du1, wg1, wu1, 6, Scatters([term_g1]), [(0, 2, 5, 7, 8)])
        dg0, du0, term_d0, (su1,) = by_hidden(by_h1, hid0, g0, u0, wd0, 7, Scatters([term_u1]), [(0, 3, 8, 11, 13)])
        term_g0, term_u0, (d0,) = by_weights(a0, dg0, du0, 8, Scatters([term_d0]), [(0, 3, 8, 11, 13)])
        sg0, su0 = scatter_all([term_g0, term_u0], 9)
        mine = [(sg0, sg1), (su0, su1), (d0, d1)]
        squares = jnp.sum(sum_of_squares([g for pair in mine for g in pair], 10))
        gradients = [jnp.stack(pair).astype(F32) for pair in mine]
        factor = jnp.minimum(1.0, 0.5 * lax.rsqrt(squares / (16 * sum(g.size for g in gradients)) + 1e-30))
        new = [adamw(w.astype(F32), m, v, g * factor) for w, m, v, g in zip(weights, m, v, gradients, strict=True)]
        return tuple(one[which] for which in range(3) for one in new)

    states, cut = P(("rep", "dp"), None, None), P(None, "dp", None)
    return jax.shard_map(
        step,
        mesh=mesh,
        in_specs=(states, states) + (cut,) * 9,
        out_specs=(P("rep", "dp", None),) * 9,
        check_vma=False,
    )
```
